32 devices in a mesh: rep: 4 (over x, y), dp: 8 (over z, core).
Axes of the slice: x: 2, y: 2, z: 4, core: 2. Of those that a mesh axis runs over, the one named last changes fastest.
Arguments:
- g_w_gate: bfloat16 [32, 2, 1024, 3072], P(('rep', 'dp')), parts along dimension 0
- g_w_up: bfloat16 [32, 2, 1024, 3072], P(('rep', 'dp')), parts along dimension 0
- g_w_down: bfloat16 [32, 2, 3072, 1024], P(('rep', 'dp')), parts along dimension 0
- w_gate: bfloat16 [2, 1024, 3072], replicated
- w_up: bfloat16 [2, 1024, 3072], replicated
- w_down: bfloat16 [2, 3072, 1024], replicated
- m_w_gate: float32 [2, 1024, 3072], P(None, 'dp')
- m_w_up: float32 [2, 1024, 3072], P(None, 'dp')
- m_w_down: float32 [2, 3072, 1024], P(None, 'dp')
- v_w_gate: float32 [2, 1024, 3072], P(None, 'dp')
- v_w_up: float32 [2, 1024, 3072], P(None, 'dp')
- v_w_down: float32 [2, 3072, 1024], P(None, 'dp')
Outputs:
- output 1: bfloat16 [8, 1024, 3072], P('rep'), parts along dimension 0
- output 2: bfloat16 [8, 1024, 3072], P('rep'), parts along dimension 0
- output 3: bfloat16 [8, 3072, 1024], P('rep'), parts along dimension 0
- output 4: float32 [8, 1024, 3072], P('rep', 'dp'), parts along dimension 0
- output 5: float32 [8, 1024, 3072], P('rep', 'dp'), parts along dimension 0
- output 6: float32 [8, 3072, 1024], P('rep', 'dp'), parts along dimension 0
- output 7: float32 [8, 1024, 3072], P('rep', 'dp'), parts along dimension 0
- output 8: float32 [8, 1024, 3072], P('rep', 'dp'), parts along dimension 0
- output 9: float32 [8, 3072, 1024], P('rep', 'dp'), parts along dimension 0
There are 4 independent parts. The reference program is written for one: setup_inputs(seed, part) draws one part's arguments, and reference() takes and returns one part's arrays. A program takes and returns all parts, laid end to end along the dimension named above; an argument that names none is the same for every part.
All inputs are finite; a program needn't handle non-finite values.
Results may differ from the reference program's by a relative error of at most 0.022.
Values are sent between devices in bfloat16 or wider.
A program may use at most 2 GiB of HBM per device.

```python
import jax
import jax.numpy as jnp
from jax import lax

DEVICES = 8
D = 1024
FF = 3072
LAYERS = 2
NAMES = ("w_gate", "w_up", "w_down")
SHAPES = {"w_gate": (LAYERS, D, FF), "w_up": (LAYERS, D, FF), "w_down": (LAYERS, FF, D)}


def setup_inputs(seed: int = 0, part: int = 0) -> dict:
    kz, *keys = jax.random.split(jax.random.key(seed), 1 + 5 * len(NAMES))
    loud = 2.0 ** jax.random.uniform(kz, (), jnp.float32, -1.0, 1.0)
    drawn = {}
    for name, key, both in zip(NAMES, keys[:3], keys[3:6], strict=True):
        own = jax.random.normal(jax.random.fold_in(key, part), (DEVICES, *SHAPES[name]), jnp.float32)
        shared = jax.random.normal(jax.random.fold_in(both, part), SHAPES[name], jnp.float32)
        drawn["g_" + name] = (loud * (0.7 * shared / DEVICES + 0.7 * own * DEVICES**-0.5)).astype(jnp.bfloat16)
    for name, key in zip(NAMES, keys[6:9], strict=True):
        drawn[name] = (jax.random.normal(key, SHAPES[name], jnp.float32) * SHAPES[name][1] ** -0.5).astype(jnp.bfloat16)
    for name, key in zip(NAMES, keys[9:12], strict=True):
        drawn["m_" + name] = loud * 0.5 * jax.random.normal(key, SHAPES[name], jnp.float32)
    for name, key in zip(NAMES, keys[12:15], strict=True):
        drawn["v_" + name] = loud * loud * jax.random.uniform(key, SHAPES[name], jnp.float32, 0.5, 1.5)
    return drawn


def adamw(w, m, v, g):
    m = 0.9 * m + 0.1 * g
    v = 0.95 * v + 0.05 * g * g
    step = m * lax.rsqrt(v + 1e-8) + 0.1 * w
    return (w - 0.02 * step).astype(jnp.bfloat16), m, v


def reference(g_w_gate, g_w_up, g_w_down, w_gate, w_up, w_down, m_w_gate, m_w_up, m_w_down, v_w_gate, v_w_up, v_w_down):
    def total(terms):
        return lax.scan(lambda so_far, term: (so_far + term.astype(jnp.float32), None), jnp.zeros(terms.shape[1:], jnp.float32), terms)[0]

    gradients = [total(terms).astype(jnp.bfloat16).astype(jnp.float32) for terms in (g_w_gate, g_w_up, g_w_down)]
    new = [
        adamw(w.astype(jnp.float32), m, v, g)
        for w, m, v, g in zip((w_gate, w_up, w_down), (m_w_gate, m_w_up, m_w_down), (v_w_gate, v_w_up, v_w_down), gradients, strict=True)
    ]
    return tuple(one[which] for which in range(3) for one in new)
```

```python
import functools

import jax
import jax.numpy as jnp
from jax import lax
from jax.experimental import pallas as pl
from jax.experimental.pallas import tpu as pltpu
from jax.sharding import PartitionSpec as P

MESH = pl.DeviceIdType.MESH
CHIPS = 4
COLS = 1024
ROWS = 64
LAG = 1
AHEAD = 2
OWN = AHEAD + 3 * LAG + 1
SLOTS = 4
BAND = 16


def piece(j, per, r, cols):
    layer = j // (per // 2)
    k = j % (per // 2)
    across = cols // COLS
    return layer, pl.multiple_of((k // across) * ROWS, ROWS), pl.multiple_of((k % across) * COLS, COLS)


def kernel(steps, *refs):
    g, w, m, v, wo, mo, vo = (refs[i : i + 3] for i in range(0, 21, 3))
    (own, theirs, right, left, w_in, m_in, v_in, w_new, m_new, v_new,
     own_sem, theirs_send, theirs_recv, right_send, right_recv, left_send, left_recv,
     in_sem, mv_sem, new_sem, relay_right, relay_left, relay_core, gather_right, gather_left, gather_core) = refs[21:]
    per = steps // 3
    rep, me = lax.axis_index("rep"), lax.axis_index("dp")
    z, c = me // 2, me % 2
    last = CHIPS - 1
    partner, up, down = (rep, me + 1 - 2 * c), (rep, me + 2), (rep, me - 2)

    barrier = pltpu.get_barrier_semaphore()
    pl.semaphore_signal(barrier, inc=1, device_id=partner, device_id_type=MESH)

    @pl.when(z < last)
    def _():
        pl.semaphore_signal(barrier, inc=1, device_id=up, device_id_type=MESH)

    @pl.when(z > 0)
    def _():
        pl.semaphore_signal(barrier, inc=1, device_id=down, device_id_type=MESH)

    pl.semaphore_wait(barrier, 1 + jnp.minimum(z, 1) + jnp.minimum(last - z, 1))

    def remote(src, dst, send, recv, to):
        return pltpu.make_async_remote_copy(src_ref=src, dst_ref=dst, send_sem=send, recv_sem=recv, device_id=to, device_id_type=MESH)

    def each_weight(j, do):
        for k in range(3):

            @pl.when((j >= k * per) & (j < (k + 1) * per))
            def _(k=k):
                layer, row, col = piece(j - k * per, per, m[k].shape[1], m[k].shape[2])
                do(k, layer, pl.ds(row, ROWS), pl.ds(col, COLS))

    def load_terms(j):
        def do(k, layer, rows, cols):
            remote(g[k].at[layer, :, 1 - c, rows, cols], theirs.at[j], theirs_send, theirs_recv.at[j], partner).start()
            pltpu.make_async_copy(g[k].at[layer, :, c, rows, cols], own.at[j % OWN], own_sem.at[j % OWN]).start()

        each_weight(j, do)

    def load_state(j):
        s = j % SLOTS

        def do(k, layer, rows, cols):
            pltpu.make_async_copy(w[k].at[layer, z, c, rows, cols], w_in.at[s], in_sem.at[0, s]).start()
            pltpu.make_async_copy(m[k].at[layer, rows, cols], m_in.at[s], in_sem.at[1, s]).start()
            pltpu.make_async_copy(v[k].at[layer, rows, cols], v_in.at[s], in_sem.at[2, s]).start()

        each_weight(j, do)

    def bands(do):
        @pl.loop(0, ROWS // BAND)
        def _(t):
            do(pl.ds(pl.multiple_of(t * BAND, BAND), BAND))

    def forward(buf, slot, b, j, send, recv, to, first):
        @pl.when(first)
        def _():
            def do(r):
                total = own[j % OWN, b, r].astype(jnp.float32) + theirs[j, b, r].astype(jnp.float32)
                buf[slot, j, r] = total.astype(jnp.bfloat16)

            bands(do)

        @pl.when(jnp.logical_not(first))
        def _():
            remote(buf.at[slot, j], buf.at[slot, j], send.at[slot], recv.at[slot, j], to).wait_recv()

            def do(r):
                total = own[j % OWN, b, r].astype(jnp.float32) + theirs[j, b, r].astype(jnp.float32)
                buf[slot, j, r] = (total + buf[slot, j, r].astype(jnp.float32)).astype(jnp.bfloat16)

            bands(do)

        remote(buf.at[slot, j], buf.at[slot, j], send.at[slot], recv.at[slot, j], to).start()

    def new_copies(j, do):
        s = j % SLOTS

        def place(k, layer, rows, cols):
            dst = wo[k].at[layer, z, c, rows, cols]
            do(pltpu.make_async_copy(w_new.at[s], dst, new_sem.at[0, s]))
            do(remote(w_new.at[s], dst, new_sem.at[1, s], gather_core.at[k], partner))

            @pl.when(z < last)
            def _():
                do(remote(w_new.at[s], dst, new_sem.at[2, s], gather_right.at[jnp.minimum(z, 2), j], up))

            @pl.when(z > 0)
            def _():
                do(remote(w_new.at[s], dst, new_sem.at[3, s], gather_left.at[jnp.maximum(z, 1) - 1, j], down))

            do(pltpu.make_async_copy(m_new.at[s], mo[k].at[layer, rows, cols], mv_sem.at[0, s]))
            do(pltpu.make_async_copy(v_new.at[s], vo[k].at[layer, rows, cols], mv_sem.at[1, s]))

        each_weight(j, place)

    def wait_new(j):
        def do(copy):
            if copy.is_remote:
                copy.wait_send()
            else:
                copy.wait()

        new_copies(j, do)

    def step(j, with_right, with_left):
        s = j % SLOTS

        def do(r):
            total = own[j % OWN, z, r].astype(jnp.float32) + theirs[j, z, r].astype(jnp.float32)
            if with_right:
                total += right[jnp.maximum(z, 1) - 1, j, r].astype(jnp.float32)
            if with_left:
                total += left[jnp.minimum(z, 2), j, r].astype(jnp.float32)
            grad = total.astype(jnp.bfloat16).astype(jnp.float32)
            mean = 0.9 * m_in[s, r] + 0.1 * grad
            var = 0.95 * v_in[s, r] + 0.05 * grad * grad
            weight = w_in[s, r].astype(jnp.float32)
            change = mean * lax.rsqrt(var + 1e-8) + 0.1 * weight
            w_new[s, r] = (weight - 0.02 * change).astype(jnp.bfloat16)
            m_new[s, r] = mean
            v_new[s, r] = var

        bands(do)

    def final(j):
        s = j % SLOTS

        @pl.when(j >= SLOTS)
        def _():
            wait_new(j - SLOTS)

        pltpu.make_async_copy(w[0].at[0, 0, 0, pl.ds(0, ROWS), pl.ds(0, COLS)], w_in.at[s], in_sem.at[0, s]).wait()
        pltpu.make_async_copy(m[0].at[0, pl.ds(0, ROWS), pl.ds(0, COLS)], m_in.at[s], in_sem.at[1, s]).wait()
        pltpu.make_async_copy(v[0].at[0, pl.ds(0, ROWS), pl.ds(0, COLS)], v_in.at[s], in_sem.at[2, s]).wait()

        @pl.when(z > 0)
        def _():
            slot = jnp.maximum(z, 1) - 1
            remote(right.at[slot, j], right.at[slot, j], right_send.at[slot], right_recv.at[slot, j], down).wait_recv()

        @pl.when(z < last)
        def _():
            slot = jnp.minimum(z, 2)
            remote(left.at[slot, j], left.at[slot, j], left_send.at[slot], left_recv.at[slot, j], up).wait_recv()

        @pl.when(z == 0)
        def _():
            step(j, False, True)

        @pl.when(z == last)
        def _():
            step(j, True, False)

        @pl.when((z > 0) & (z < last))
        def _():
            step(j, True, True)

        new_copies(j, lambda copy: copy.start())

        @pl.when(j + 2 < steps)
        def _():
            load_state(j + 2)

    def relay(b, j, slot, recv, sent, to, more):
        def do(k, layer, rows, cols):
            here = wo[k].at[layer, b, c, rows, cols]
            remote(here, here, sent.at[slot], recv.at[slot, j], to).wait_recv()

            @pl.when(more)
            def _():
                remote(here, here, sent.at[slot], recv.at[slot, j], to).start()

            remote(here, here, relay_core, gather_core.at[k], partner).start()

        each_weight(j, do)

    done_at = [LAG * max(b, last - b) for b in range(CHIPS)]
    mine = LAG * jnp.maximum(z, last - z)

    for j in range(AHEAD):
        load_terms(j)
    for j in range(2):
        load_state(j)

    def within(j):
        return (j >= 0) & (j < steps)

    @pl.loop(0, steps + 2 * last * LAG)
    def _(i):
        @pl.when(i + AHEAD < steps)
        def _():
            load_terms(i + AHEAD)

        @pl.when(i < steps)
        def _():
            pltpu.make_async_copy(own.at[i % OWN], own.at[i % OWN], own_sem.at[i % OWN]).wait()
            remote(theirs.at[i], theirs.at[i], theirs_send, theirs_recv.at[i], partner).wait_recv()

        j_right = i - LAG * z
        j_left = i - LAG * (last - z)
        for n in range(last):
            b = last - n

            @pl.when(within(j_right) & (b > z))
            def _(b=b):
                forward(right, b - 1, b, j_right, right_send, right_recv, up, z == 0)

            @pl.when(within(j_left) & (n < z))
            def _(n=n):
                forward(left, n, n, j_left, left_send, left_recv, down, z == last)

        j_mine = i - mine

        @pl.when(within(j_mine))
        def _():
            final(j_mine)

        for n in range(last):
            b = last - n
            j = i - done_at[n] - LAG * (z - n)

            @pl.when(within(j) & (n < z))
            def _(n=n, j=j):
                relay(n, j, n, gather_right, relay_right, up, z < last)

            j = i - done_at[b] - LAG * (b - z)

            @pl.when(within(j) & (b > z))
            def _(b=b, j=j):
                relay(b, j, b - 1, gather_left, relay_left, down, z > 0)

    for j in range(steps - SLOTS, steps):
        wait_new(j)
    remote(theirs, theirs, theirs_send, theirs_recv.at[0], partner).wait_send()
    remote(right, right, relay_core, theirs_recv.at[0], partner).wait_send()
    for n in range(last):
        b = last - n

        @pl.when(b > z)
        def _(b=b):
            remote(right.at[0], right.at[0], right_send.at[b - 1], theirs_recv.at[0], up).wait_send()

        @pl.when(n < z)
        def _(n=n):
            remote(left.at[0], left.at[0], left_send.at[n], theirs_recv.at[0], down).wait_send()

        @pl.when((n < z) & (z < last))
        def _(n=n):
            remote(right.at[0], right.at[0], relay_right.at[n], theirs_recv.at[0], up).wait_send()

        @pl.when((b > z) & (z > 0))
        def _(b=b):
            remote(left.at[0], left.at[0], relay_left.at[b - 1], theirs_recv.at[0], down).wait_send()

    for k in range(3):
        arrived = wo[k].at[:, :, 1 - c]
        remote(arrived, arrived, theirs_send, gather_core.at[k], partner).wait_recv()


def solution(mesh):
    cores = mesh.shape["dp"] // CHIPS

    def step(*arrays):
        terms, weights, m, v = (arrays[i : i + 3] for i in (0, 3, 6, 9))
        steps = 3 * m[0].size // (ROWS * COLS)
        split = lambda a, one: a.reshape(one.shape[0], CHIPS, cores, *one.shape[1:])
        g = [split(a, one) for a, one in zip(terms, m, strict=True)]
        w = [split(a, one) for a, one in zip(weights, m, strict=True)]
        any_space = pl.BlockSpec(memory_space=pl.ANY)
        dma = pltpu.SemaphoreType.DMA
        half, full = jnp.bfloat16, jnp.float32
        outs = [jax.ShapeDtypeStruct(a.shape, a.dtype) for a in (*w, *m, *v)]
        got = pl.pallas_call(
            functools.partial(kernel, steps),
            out_shape=outs,
            in_specs=[any_space] * 12,
            out_specs=[any_space] * 9,
            scratch_shapes=[
                pltpu.VMEM((OWN, CHIPS, ROWS, COLS), half),
                pltpu.VMEM((steps, CHIPS, ROWS, COLS), half),
                pltpu.VMEM((CHIPS - 1, steps, ROWS, COLS), half),
                pltpu.VMEM((CHIPS - 1, steps, ROWS, COLS), half),
                pltpu.VMEM((SLOTS, ROWS, COLS), half),
                pltpu.VMEM((SLOTS, ROWS, COLS), full),
                pltpu.VMEM((SLOTS, ROWS, COLS), full),
                pltpu.VMEM((SLOTS, ROWS, COLS), half),
                pltpu.VMEM((SLOTS, ROWS, COLS), full),
                pltpu.VMEM((SLOTS, ROWS, COLS), full),
                dma((OWN,)),
                dma,
                dma((steps,)),
                dma((CHIPS - 1,)),
                dma((CHIPS - 1, steps)),
                dma((CHIPS - 1,)),
                dma((CHIPS - 1, steps)),
                dma((3, SLOTS)),
                dma((2, SLOTS)),
                dma((4, SLOTS)),
                dma((CHIPS - 1,)),
                dma((CHIPS - 1,)),
                dma,
                dma((CHIPS - 1, steps)),
                dma((CHIPS - 1, steps)),
                dma((3,)),
            ],
            compiler_params=pltpu.CompilerParams(collective_id=0, has_side_effects=True, vmem_limit_bytes=67_000_000),
            name="sum_step_gather",
        )(*g, *w, *m, *v)
        whole = [a.reshape(b.shape) for a, b in zip(got[:3], weights, strict=True)]
        return (*whole, *got[3:])

    all_of, cut = P(None, None, None), P(None, "dp", None)
    return jax.shard_map(
        step,
        mesh=mesh,
        in_specs=(P(("rep", "dp"), None, None, None),) * 3 + (all_of,) * 3 + (cut,) * 6,
        out_specs=(P("rep", None, None),) * 3 + (P("rep", "dp", None),) * 6,
        check_vma=False,
    )
```

```python
import functools

import jax
import jax.numpy as jnp
from jax import lax
from jax.experimental import pallas as pl
from jax.experimental.pallas import tpu as pltpu
from jax.sharding import PartitionSpec as P

MESH = pl.DeviceIdType.MESH
CHIPS = 4
COLS = 1024
ROWS = 32
LAG = 1
AHEAD = 2
OWN = AHEAD + 3 * LAG + 1
SLOTS = 4
THEIRS = OWN + 2
CHUNKS = 8
BAND = 16


def piece(j, per, r, cols):
    layer = j // (per // 2)
    k = j % (per // 2)
    across = cols // COLS
    return layer, pl.multiple_of((k // across) * ROWS, ROWS), pl.multiple_of((k % across) * COLS, COLS)


def kernel(steps, *refs):
    g, w, m, v, wo = (refs[i : i + 3] for i in range(0, 15, 3))
    (m_new, v_new, own, theirs, right, left, w_in, m_in, v_in, w_new,
     own_sem, theirs_send, theirs_recv, theirs_free, right_send, right_recv, left_send, left_recv,
     in_sem, new_sem, relay_right, relay_left, relay_core, gather_right, gather_left, gather_core) = refs[15:]
    per = steps // 3
    rep, me = lax.axis_index("rep"), lax.axis_index("dp")
    z, c = me // 2, me % 2
    last = CHIPS - 1
    partner, up, down = (rep, me + 1 - 2 * c), (rep, me + 2), (rep, me - 2)

    barrier = pltpu.get_barrier_semaphore()
    pl.semaphore_signal(barrier, inc=1, device_id=partner, device_id_type=MESH)

    @pl.when(z < last)
    def _():
        pl.semaphore_signal(barrier, inc=1, device_id=up, device_id_type=MESH)

    @pl.when(z > 0)
    def _():
        pl.semaphore_signal(barrier, inc=1, device_id=down, device_id_type=MESH)

    pl.semaphore_wait(barrier, 1 + jnp.minimum(z, 1) + jnp.minimum(last - z, 1))

    def remote(src, dst, send, recv, to):
        return pltpu.make_async_remote_copy(src_ref=src, dst_ref=dst, send_sem=send, recv_sem=recv, device_id=to, device_id_type=MESH)

    def each_weight(j, do):
        for k in range(3):

            @pl.when((j >= k * per) & (j < (k + 1) * per))
            def _(k=k):
                layer, row, col = piece(j - k * per, per, m[k].shape[1], m[k].shape[2])
                do(k, layer, pl.ds(row, ROWS), pl.ds(col, COLS))

    def load_terms(j):
        t = j % THEIRS

        @pl.when(j >= THEIRS)
        def _():
            pl.semaphore_wait(theirs_free, 1)

        def do(k, layer, rows, cols):
            remote(g[k].at[layer, :, 1 - c, rows, cols], theirs.at[t], theirs_send, theirs_recv.at[t], partner).start()
            pltpu.make_async_copy(g[k].at[layer, :, c, rows, cols], own.at[j % OWN], own_sem.at[j % OWN]).start()

        each_weight(j, do)

    def load_state(j):
        s = j % SLOTS

        def do(k, layer, rows, cols):
            pltpu.make_async_copy(w[k].at[layer, z, c, rows, cols], w_in.at[s], in_sem.at[0, s]).start()
            pltpu.make_async_copy(m[k].at[layer, rows, cols], m_in.at[s], in_sem.at[1, s]).start()
            pltpu.make_async_copy(v[k].at[layer, rows, cols], v_in.at[s], in_sem.at[2, s]).start()

        each_weight(j, do)

    def bands(do):
        @pl.loop(0, ROWS // BAND)
        def _(t):
            do(pl.ds(pl.multiple_of(t * BAND, BAND), BAND))

    def forward(buf, slot, b, j, send, recv, to, first):
        @pl.when(first)
        def _():
            def do(r):
                total = own[j % OWN, b, r].astype(jnp.float32) + theirs[j % THEIRS, b, r].astype(jnp.float32)
                buf[slot, j, r] = total.astype(jnp.bfloat16)

            bands(do)

        @pl.when(jnp.logical_not(first))
        def _():
            remote(buf.at[slot, j], buf.at[slot, j], send.at[slot], recv.at[slot, j], to).wait_recv()

            def do(r):
                total = own[j % OWN, b, r].astype(jnp.float32) + theirs[j % THEIRS, b, r].astype(jnp.float32)
                buf[slot, j, r] = (total + buf[slot, j, r].astype(jnp.float32)).astype(jnp.bfloat16)

            bands(do)

        remote(buf.at[slot, j], buf.at[slot, j], send.at[slot], recv.at[slot, j], to).start()

    def new_copies(j, do):
        s = j % SLOTS

        def place(k, layer, rows, cols):
            dst = wo[k].at[layer, z, c, rows, cols]
            do(pltpu.make_async_copy(w_new.at[s], dst, new_sem.at[0, s]))
            do(remote(w_new.at[s], dst, new_sem.at[1, s], gather_core.at[k], partner))

            @pl.when(z < last)
            def _():
                do(remote(w_new.at[s], dst, new_sem.at[2, s], gather_right.at[jnp.minimum(z, 2), j], up))

            @pl.when(z > 0)
            def _():
                do(remote(w_new.at[s], dst, new_sem.at[3, s], gather_left.at[jnp.maximum(z, 1) - 1, j], down))

        each_weight(j, place)

    def wait_new(j):
        def do(copy):
            if copy.is_remote:
                copy.wait_send()
            else:
                copy.wait()

        new_copies(j, do)

    def step(j, with_right, with_left):
        s = j % SLOTS

        def do(r):
            total = own[j % OWN, z, r].astype(jnp.float32) + theirs[j % THEIRS, z, r].astype(jnp.float32)
            if with_right:
                total += right[jnp.maximum(z, 1) - 1, j, r].astype(jnp.float32)
            if with_left:
                total += left[jnp.minimum(z, 2), j, r].astype(jnp.float32)
            grad = total.astype(jnp.bfloat16).astype(jnp.float32)
            mean = 0.9 * m_in[s, r] + 0.1 * grad
            var = 0.95 * v_in[s, r] + 0.05 * grad * grad
            weight = w_in[s, r].astype(jnp.float32)
            change = mean * lax.rsqrt(var + 1e-8) + 0.1 * weight
            w_new[s, r] = (weight - 0.02 * change).astype(jnp.bfloat16)
            m_new[j, r] = mean
            v_new[j, r] = var

        bands(do)

    def final(j):
        s = j % SLOTS

        @pl.when(j >= SLOTS)
        def _():
            wait_new(j - SLOTS)

        pltpu.make_async_copy(w[0].at[0, 0, 0, pl.ds(0, ROWS), pl.ds(0, COLS)], w_in.at[s], in_sem.at[0, s]).wait()
        pltpu.make_async_copy(m[0].at[0, pl.ds(0, ROWS), pl.ds(0, COLS)], m_in.at[s], in_sem.at[1, s]).wait()
        pltpu.make_async_copy(v[0].at[0, pl.ds(0, ROWS), pl.ds(0, COLS)], v_in.at[s], in_sem.at[2, s]).wait()

        @pl.when(z > 0)
        def _():
            slot = jnp.maximum(z, 1) - 1
            remote(right.at[slot, j], right.at[slot, j], right_send.at[slot], right_recv.at[slot, j], down).wait_recv()

        @pl.when(z < last)
        def _():
            slot = jnp.minimum(z, 2)
            remote(left.at[slot, j], left.at[slot, j], left_send.at[slot], left_recv.at[slot, j], up).wait_recv()

        @pl.when(z == 0)
        def _():
            step(j, False, True)

        @pl.when(z == last)
        def _():
            step(j, True, False)

        @pl.when((z > 0) & (z < last))
        def _():
            step(j, True, True)

        new_copies(j, lambda copy: copy.start())

        @pl.when(j + 2 < steps)
        def _():
            load_state(j + 2)

    def relay(b, j, slot, recv, sent, to, more):
        def do(k, layer, rows, cols):
            here = wo[k].at[layer, b, c, rows, cols]
            remote(here, here, sent.at[slot], recv.at[slot, j], to).wait_recv()

            @pl.when(more)
            def _():
                remote(here, here, sent.at[slot], recv.at[slot, j], to).start()

            remote(here, here, relay_core, gather_core.at[k], partner).start()

        each_weight(j, do)

    done_at = [LAG * max(b, last - b) for b in range(CHIPS)]
    mine = LAG * jnp.maximum(z, last - z)

    for j in range(AHEAD):
        load_terms(j)
    for j in range(2):
        load_state(j)

    def within(j):
        return (j >= 0) & (j < steps)

    @pl.loop(0, steps + 2 * last * LAG)
    def _(i):
        @pl.when(i + AHEAD < steps)
        def _():
            load_terms(i + AHEAD)

        @pl.when(i < steps)
        def _():
            pltpu.make_async_copy(own.at[i % OWN], own.at[i % OWN], own_sem.at[i % OWN]).wait()
            t = i % THEIRS
            remote(theirs.at[t], theirs.at[t], theirs_send, theirs_recv.at[t], partner).wait_recv()

        j_right = i - LAG * z
        j_left = i - LAG * (last - z)
        for n in range(last):
            b = last - n

            @pl.when(within(j_right) & (b > z))
            def _(b=b):
                forward(right, b - 1, b, j_right, right_send, right_recv, up, z == 0)

            @pl.when(within(j_left) & (n < z))
            def _(n=n):
                forward(left, n, n, j_left, left_send, left_recv, down, z == last)

        j_mine = i - mine

        @pl.when(within(j_mine))
        def _():
            final(j_mine)

        j_free = i - last * LAG

        @pl.when((j_free >= 0) & (j_free < steps - THEIRS))
        def _():
            pl.semaphore_signal(theirs_free, inc=1, device_id=partner, device_id_type=MESH)

        for n in range(last):
            b = last - n
            j = i - done_at[n] - LAG * (z - n)

            @pl.when(within(j) & (n < z))
            def _(n=n, j=j):
                relay(n, j, n, gather_right, relay_right, up, z < last)

            j = i - done_at[b] - LAG * (b - z)

            @pl.when(within(j) & (b > z))
            def _(b=b, j=j):
                relay(b, j, b - 1, gather_left, relay_left, down, z > 0)

    for j in range(steps - SLOTS, steps):
        wait_new(j)
    for k in range(3):
        sent = g[k].at[:, :, 1 - c]
        remote(sent, sent, theirs_send, theirs_recv.at[0], partner).wait_send()
    remote(right, right, relay_core, theirs_recv.at[0], partner).wait_send()
    for n in range(last):
        b = last - n

        @pl.when(b > z)
        def _(b=b):
            remote(right.at[0], right.at[0], right_send.at[b - 1], theirs_recv.at[0], up).wait_send()

        @pl.when(n < z)
        def _(n=n):
            remote(left.at[0], left.at[0], left_send.at[n], theirs_recv.at[0], down).wait_send()

        @pl.when((n < z) & (z < last))
        def _(n=n):
            remote(right.at[0], right.at[0], relay_right.at[n], theirs_recv.at[0], up).wait_send()

        @pl.when((b > z) & (z > 0))
        def _(b=b):
            remote(left.at[0], left.at[0], relay_left.at[b - 1], theirs_recv.at[0], down).wait_send()

    for k in range(3):
        arrived = wo[k].at[:, :, 1 - c]
        remote(arrived, arrived, theirs_send, gather_core.at[k], partner).wait_recv()


def finish(steps, *refs):
    w, m, v = refs[:3], refs[3], refs[4]
    wo, mo, vo = (refs[i : i + 3] for i in range(5, 14, 3))
    stage, in_sem, out_sem, m_sem, v_sem = refs[14], refs[15], refs[16], refs[17], refs[18]
    per = steps // 3
    height = [a.shape[1] // (CHUNKS // 2) for a in w]

    def part(a, k, n):
        return a[k].at[n // (CHUNKS // 2), pl.ds(n % (CHUNKS // 2) * height[k], height[k])]

    def held(k, n):
        return stage[k].at[n]

    for n in range(CHUNKS):
        for k in range(3):
            pltpu.make_async_copy(part(w, k, n), held(k, n), in_sem.at[k, n]).start()

    for k in range(3):

        @pl.loop(0, per)
        def _(j, k=k):
            layer, row, col = piece(j, per, mo[k].shape[1], mo[k].shape[2])
            place = (layer, pl.ds(row, ROWS), pl.ds(col, COLS))
            pltpu.make_async_copy(m.at[k * per + j], mo[k].at[place], m_sem).start()
            pltpu.make_async_copy(v.at[k * per + j], vo[k].at[place], v_sem).start()

    for n in range(CHUNKS):
        for k in range(3):
            pltpu.make_async_copy(part(w, k, n), held(k, n), in_sem.at[k, n]).wait()
            pltpu.make_async_copy(held(k, n), part(wo, k, n), out_sem.at[k, n]).start()

    for n in range(CHUNKS):
        for k in range(3):
            pltpu.make_async_copy(held(k, n), part(wo, k, n), out_sem.at[k, n]).wait()
    pltpu.make_async_copy(m, m, m_sem).wait()
    pltpu.make_async_copy(v, v, v_sem).wait()


def solution(mesh):
    cores = mesh.shape["dp"] // CHIPS

    def step(*arrays):
        terms, weights, m, v = (arrays[i : i + 3] for i in (0, 3, 6, 9))
        steps = 3 * m[0].size // (ROWS * COLS)
        split = lambda a, one: a.reshape(one.shape[0], CHIPS, cores, *one.shape[1:])
        g = [split(a, one) for a, one in zip(terms, m, strict=True)]
        w = [split(a, one) for a, one in zip(weights, m, strict=True)]
        any_space, hbm, vmem = (pl.BlockSpec(memory_space=a) for a in (pl.ANY, pltpu.HBM, pltpu.VMEM))
        dma = pltpu.SemaphoreType.DMA
        half, full = jnp.bfloat16, jnp.float32
        state = (steps, ROWS, COLS)
        got = pl.pallas_call(
            functools.partial(kernel, steps),
            out_shape=[*(pltpu.HBM(a.shape, a.dtype) for a in w), pltpu.VMEM(state, full), pltpu.VMEM(state, full)],
            in_specs=[any_space] * 12,
            out_specs=[hbm] * 3 + [vmem] * 2,
            scratch_shapes=[
                pltpu.VMEM((OWN, CHIPS, ROWS, COLS), half),
                pltpu.VMEM((THEIRS, CHIPS, ROWS, COLS), half),
                pltpu.VMEM((CHIPS - 1, steps, ROWS, COLS), half),
                pltpu.VMEM((CHIPS - 1, steps, ROWS, COLS), half),
                pltpu.VMEM((SLOTS, ROWS, COLS), half),
                pltpu.VMEM((SLOTS, ROWS, COLS), full),
                pltpu.VMEM((SLOTS, ROWS, COLS), full),
                pltpu.VMEM((SLOTS, ROWS, COLS), half),
                dma((OWN,)),
                dma,
                dma((THEIRS,)),
                pltpu.SemaphoreType.REGULAR,
                dma((CHIPS - 1,)),
                dma((CHIPS - 1, steps)),
                dma((CHIPS - 1,)),
                dma((CHIPS - 1, steps)),
                dma((3, SLOTS)),
                dma((4, SLOTS)),
                dma((CHIPS - 1,)),
                dma((CHIPS - 1,)),
                dma,
                dma((CHIPS - 1, steps)),
                dma((CHIPS - 1, steps)),
                dma((3,)),
            ],
            compiler_params=pltpu.CompilerParams(collective_id=0, has_side_effects=True, vmem_limit_bytes=46_000_000),
            name="sum_step_gather",
        )(*g, *w, *m, *v)
        new = [pltpu.with_memory_space_constraint(a.reshape(b.shape), pltpu.HBM) for a, b in zip(got[:3], weights, strict=True)]
        mv = [pltpu.with_memory_space_constraint(a, pltpu.VMEM) for a in got[3:]]
        stage = [pltpu.VMEM((CHUNKS, a.shape[1] // (CHUNKS // 2), a.shape[2]), half) for a in weights]
        return pl.pallas_call(
            functools.partial(finish, steps),
            out_shape=[pltpu.HBM(a.shape, a.dtype) for a in (*weights, *m, *v)],
            in_specs=[hbm] * 3 + [vmem] * 2,
            out_specs=[hbm] * 9,
            scratch_shapes=[stage, dma((3, CHUNKS)), dma((3, CHUNKS)), dma, dma],
            compiler_params=pltpu.CompilerParams(vmem_limit_bytes=46_000_000),
            name="finish",
        )(*new, *mv)

    all_of, cut = P(None, None, None), P(None, "dp", None)
    return jax.shard_map(
        step,
        mesh=mesh,
        in_specs=(P(("rep", "dp"), None, None, None),) * 3 + (all_of,) * 3 + (cut,) * 6,
        out_specs=(P("rep", None, None),) * 3 + (P("rep", "dp", None),) * 6,
        check_vma=False,
    )
```

```python
import functools

import jax
import jax.numpy as jnp
from jax import lax
from jax.experimental import pallas as pl
from jax.experimental.pallas import tpu as pltpu
from jax.sharding import PartitionSpec as P

MESH = pl.DeviceIdType.MESH
CHIPS = 4
COLS = 1024
ROWS = 32
LAG = 1
AHEAD = 2
OWN = AHEAD + 3 * LAG + 1
SLOTS = 4
THEIRS = OWN + 2
RING = 8
GRANT = 9_400_000
BAND = 16


def piece(j, per, r, cols):
    layer = j // (per // 2)
    k = j % (per // 2)
    across = cols // COLS
    return layer, pl.multiple_of((k // across) * ROWS, ROWS), pl.multiple_of((k % across) * COLS, COLS)


def kernel(steps, *refs):
    g, w, m, v, wo = (refs[i : i + 3] for i in range(0, 15, 3))
    (m_new, v_new, own, theirs, right, left, w_in, m_in, v_in,
     own_sem, theirs_send, theirs_recv, theirs_free, right_send, right_recv, right_free, left_send, left_recv, left_free,
     in_sem, new_sem, relay_right, relay_left, relay_core, gather_right, gather_left, gather_core) = refs[15:]
    per = steps // 3
    rep, me = lax.axis_index("rep"), lax.axis_index("dp")
    z, c = me // 2, me % 2
    last = CHIPS - 1
    partner, up, down = (rep, me + 1 - 2 * c), (rep, me + 2), (rep, me - 2)

    barrier = pltpu.get_barrier_semaphore()
    pl.semaphore_signal(barrier, inc=1, device_id=partner, device_id_type=MESH)

    @pl.when(z < last)
    def _():
        pl.semaphore_signal(barrier, inc=1, device_id=up, device_id_type=MESH)

    @pl.when(z > 0)
    def _():
        pl.semaphore_signal(barrier, inc=1, device_id=down, device_id_type=MESH)

    pl.semaphore_wait(barrier, 1 + jnp.minimum(z, 1) + jnp.minimum(last - z, 1))

    def remote(src, dst, send, recv, to):
        return pltpu.make_async_remote_copy(src_ref=src, dst_ref=dst, send_sem=send, recv_sem=recv, device_id=to, device_id_type=MESH)

    def each_weight(j, do):
        for k in range(3):

            @pl.when((j >= k * per) & (j < (k + 1) * per))
            def _(k=k):
                layer, row, col = piece(j - k * per, per, m[k].shape[1], m[k].shape[2])
                do(k, layer, pl.ds(row, ROWS), pl.ds(col, COLS))

    def load_terms(j):
        t = j % THEIRS

        @pl.when(j >= THEIRS)
        def _():
            pl.semaphore_wait(theirs_free, 1)

        def do(k, layer, rows, cols):
            remote(g[k].at[layer, :, 1 - c, rows, cols], theirs.at[t], theirs_send, theirs_recv.at[t], partner).start()
            pltpu.make_async_copy(g[k].at[layer, :, c, rows, cols], own.at[j % OWN], own_sem.at[j % OWN]).start()

        each_weight(j, do)

    def load_state(j):
        s = j % SLOTS

        def do(k, layer, rows, cols):
            pltpu.make_async_copy(w[k].at[layer, z, c, rows, cols], w_in.at[s], in_sem.at[0, s]).start()
            pltpu.make_async_copy(m[k].at[layer, rows, cols], m_in.at[s], in_sem.at[1, s]).start()
            pltpu.make_async_copy(v[k].at[layer, rows, cols], v_in.at[s], in_sem.at[2, s]).start()

        each_weight(j, do)

    def bands(do):
        @pl.loop(0, ROWS // BAND)
        def _(t):
            do(pl.ds(pl.multiple_of(t * BAND, BAND), BAND))

    def forward(buf, slot, b, j, send, recv, to, first):
        q = j % RING

        @pl.when(first)
        def _():
            def do(r):
                total = own[j % OWN, b, r].astype(jnp.float32) + theirs[j % THEIRS, b, r].astype(jnp.float32)
                buf[slot, q, r] = total.astype(jnp.bfloat16)

            bands(do)

        @pl.when(jnp.logical_not(first))
        def _():
            remote(buf.at[slot, q], buf.at[slot, q], send.at[slot, q], recv.at[slot, q], to).wait_recv()

            def do(r):
                total = own[j % OWN, b, r].astype(jnp.float32) + theirs[j % THEIRS, b, r].astype(jnp.float32)
                buf[slot, q, r] = (total + buf[slot, q, r].astype(jnp.float32)).astype(jnp.bfloat16)

            bands(do)

        remote(buf.at[slot, q], buf.at[slot, q], send.at[slot, q], recv.at[slot, q], to).start()

    def step(j, k, layer, rows, cols, with_right, with_left):
        s, q = j % SLOTS, j % RING

        def do(r):
            total = own[j % OWN, z, r].astype(jnp.float32) + theirs[j % THEIRS, z, r].astype(jnp.float32)
            if with_right:
                total += right[jnp.maximum(z, 1) - 1, q, r].astype(jnp.float32)
            if with_left:
                total += left[jnp.minimum(z, 2), q, r].astype(jnp.float32)
            grad = total.astype(jnp.bfloat16).astype(jnp.float32)
            mean = 0.9 * m_in[s, r] + 0.1 * grad
            var = 0.95 * v_in[s, r] + 0.05 * grad * grad
            weight = w_in[s, r].astype(jnp.float32)
            change = mean * lax.rsqrt(var + 1e-8) + 0.1 * weight
            place = pl.ds(pl.multiple_of(rows.start + r.start, BAND), BAND)
            wo[k][layer, z, c, place, cols] = (weight - 0.02 * change).astype(jnp.bfloat16)
            m_new[j, r] = mean
            v_new[j, r] = var

        bands(do)

    def final(j):
        s, q = j % SLOTS, j % RING
        pltpu.make_async_copy(w[0].at[0, 0, 0, pl.ds(0, ROWS), pl.ds(0, COLS)], w_in.at[s], in_sem.at[0, s]).wait()
        pltpu.make_async_copy(m[0].at[0, pl.ds(0, ROWS), pl.ds(0, COLS)], m_in.at[s], in_sem.at[1, s]).wait()
        pltpu.make_async_copy(v[0].at[0, pl.ds(0, ROWS), pl.ds(0, COLS)], v_in.at[s], in_sem.at[2, s]).wait()

        @pl.when(z > 0)
        def _():
            slot = jnp.maximum(z, 1) - 1
            remote(right.at[slot, q], right.at[slot, q], right_send.at[slot, q], right_recv.at[slot, q], down).wait_recv()

        @pl.when(z < last)
        def _():
            slot = jnp.minimum(z, 2)
            remote(left.at[slot, q], left.at[slot, q], left_send.at[slot, q], left_recv.at[slot, q], up).wait_recv()

        def do(k, layer, rows, cols):
            @pl.when(z == 0)
            def _():
                step(j, k, layer, rows, cols, False, True)

            @pl.when(z == last)
            def _():
                step(j, k, layer, rows, cols, True, False)

            @pl.when((z > 0) & (z < last))
            def _():
                step(j, k, layer, rows, cols, True, True)

            here = wo[k].at[layer, z, c, rows, cols]

            @pl.when(z < last)
            def _():
                remote(here, here, new_sem.at[0], gather_right.at[jnp.minimum(z, 2), j], up).start()

            @pl.when(z > 0)
            def _():
                remote(here, here, new_sem.at[1], gather_left.at[jnp.maximum(z, 1) - 1, j], down).start()

            remote(here, here, new_sem.at[2], gather_core.at[k], partner).start()

        each_weight(j, do)

        @pl.when(j + 2 < steps)
        def _():
            load_state(j + 2)

    def retire(j):
        q = j % RING
        for n in range(last):
            b = last - n

            @pl.when(b > z)
            def _(b=b):
                remote(right.at[b - 1, q], right.at[b - 1, q], right_send.at[b - 1, q], right_recv.at[b - 1, q], up).wait_send()

            @pl.when(n < z)
            def _(n=n):
                remote(left.at[n, q], left.at[n, q], left_send.at[n, q], left_recv.at[n, q], down).wait_send()

        @pl.when((j < steps - RING) & (z > 0))
        def _():
            pl.semaphore_signal(right_free, inc=1, device_id=down, device_id_type=MESH)

        @pl.when((j < steps - RING) & (z < last))
        def _():
            pl.semaphore_signal(left_free, inc=1, device_id=up, device_id_type=MESH)

    def relay(b, j, slot, recv, sent, to, more):
        def do(k, layer, rows, cols):
            here = wo[k].at[layer, b, c, rows, cols]
            remote(here, here, sent.at[slot], recv.at[slot, j], to).wait_recv()

            @pl.when(more)
            def _():
                remote(here, here, sent.at[slot], recv.at[slot, j], to).start()

            remote(here, here, relay_core, gather_core.at[k], partner).start()

        each_weight(j, do)

    done_at = [LAG * max(b, last - b) for b in range(CHIPS)]
    mine = LAG * jnp.maximum(z, last - z)

    for j in range(AHEAD):
        load_terms(j)
    for j in range(2):
        load_state(j)

    def within(j):
        return (j >= 0) & (j < steps)

    @pl.loop(0, steps + 2 * last * LAG)
    def _(i):
        @pl.when(i + AHEAD < steps)
        def _():
            load_terms(i + AHEAD)

        @pl.when(i < steps)
        def _():
            pltpu.make_async_copy(own.at[i % OWN], own.at[i % OWN], own_sem.at[i % OWN]).wait()
            t = i % THEIRS
            remote(theirs.at[t], theirs.at[t], theirs_send, theirs_recv.at[t], partner).wait_recv()

        j_right = i - LAG * z
        j_left = i - LAG * (last - z)
        j_old = i - mine - 1

        @pl.when(within(j_old))
        def _():
            retire(j_old)

        @pl.when((j_right >= RING) & (j_right < steps) & (z < last))
        def _():
            pl.semaphore_wait(right_free, 1)

        @pl.when((j_left >= RING) & (j_left < steps) & (z > 0))
        def _():
            pl.semaphore_wait(left_free, 1)

        for n in range(last):
            b = last - n

            @pl.when(within(j_right) & (b > z))
            def _(b=b):
                forward(right, b - 1, b, j_right, right_send, right_recv, up, z == 0)

            @pl.when(within(j_left) & (n < z))
            def _(n=n):
                forward(left, n, n, j_left, left_send, left_recv, down, z == last)

        j_mine = i - mine

        @pl.when(within(j_mine))
        def _():
            final(j_mine)

        j_free = i - last * LAG

        @pl.when((j_free >= 0) & (j_free < steps - THEIRS))
        def _():
            pl.semaphore_signal(theirs_free, inc=1, device_id=partner, device_id_type=MESH)

        for n in range(last):
            b = last - n
            j = i - done_at[n] - LAG * (z - n)

            @pl.when(within(j) & (n < z))
            def _(n=n, j=j):
                relay(n, j, n, gather_right, relay_right, up, z < last)

            j = i - done_at[b] - LAG * (b - z)

            @pl.when(within(j) & (b > z))
            def _(b=b, j=j):
                relay(b, j, b - 1, gather_left, relay_left, down, z > 0)

    for k in range(3):
        sent = g[k].at[:, :, 1 - c]
        remote(sent, sent, theirs_send, gather_core.at[k], partner).wait_send()
        one = wo[k].at[:, 0, 0]
        for _ in range(last):
            remote(one, one, relay_core, gather_core.at[k], partner).wait_send()
        remote(one, one, new_sem.at[2], gather_core.at[k], partner).wait_send()

        @pl.when(z < last)
        def _():
            remote(one, one, new_sem.at[0], gather_core.at[k], up).wait_send()

        @pl.when(z > 0)
        def _():
            remote(one, one, new_sem.at[1], gather_core.at[k], down).wait_send()

        for n in range(last):
            b = last - n

            @pl.when((n < z) & (z < last))
            def _(n=n):
                remote(one, one, relay_right.at[n], gather_core.at[k], up).wait_send()

            @pl.when((b > z) & (z > 0))
            def _(b=b):
                remote(one, one, relay_left.at[b - 1], gather_core.at[k], down).wait_send()

    for k in range(3):
        arrived = wo[k].at[:, :, 1 - c]
        remote(arrived, arrived, theirs_send, gather_core.at[k], partner).wait_recv()


def finish(steps, *refs):
    w, m, v = refs[:3], refs[3], refs[4]
    wo, mo, vo = (refs[i : i + 3] for i in range(5, 14, 3))
    w_sem, m_sem, v_sem = refs[14:]
    per = steps // 3
    for k in range(3):
        layers, chips, cores, r, _ = w[k].shape

        @pl.loop(0, layers * chips * cores)
        def _(n, k=k, each=chips * cores, cores=cores, r=r):
            layer, b = n // each, n % each
            rows = pl.ds(pl.multiple_of(b * r, r), r)
            pltpu.make_async_copy(w[k].at[layer, b // cores, b % cores], wo[k].at[layer, rows], w_sem.at[k]).start()

        @pl.loop(0, per)
        def _(j, k=k):
            layer, row, col = piece(j, per, mo[k].shape[1], mo[k].shape[2])
            place = (layer, pl.ds(row, ROWS), pl.ds(col, COLS))
            pltpu.make_async_copy(m.at[k * per + j], mo[k].at[place], m_sem).start()
            pltpu.make_async_copy(v.at[k * per + j], vo[k].at[place], v_sem).start()

    for k in range(3):
        pltpu.make_async_copy(w[k], w[k], w_sem.at[k]).wait()
    pltpu.make_async_copy(m, m, m_sem).wait()
    pltpu.make_async_copy(v, v, v_sem).wait()


def solution(mesh):
    cores = mesh.shape["dp"] // CHIPS

    def step(*arrays):
        terms, weights, m, v = (arrays[i : i + 3] for i in (0, 3, 6, 9))
        steps = 3 * m[0].size // (ROWS * COLS)
        split = lambda a, one: a.reshape(one.shape[0], CHIPS, cores, *one.shape[1:])
        g = [split(a, one) for a, one in zip(terms, m, strict=True)]
        w = [split(a, one) for a, one in zip(weights, m, strict=True)]
        any_space, hbm, vmem = (pl.BlockSpec(memory_space=a) for a in (pl.ANY, pltpu.HBM, pltpu.VMEM))
        dma = pltpu.SemaphoreType.DMA
        half, full = jnp.bfloat16, jnp.float32
        state = (steps, ROWS, COLS)
        got = pl.pallas_call(
            functools.partial(kernel, steps),
            out_shape=[*(pltpu.VMEM(a.shape, a.dtype) for a in w), pltpu.VMEM(state, full), pltpu.VMEM(state, full)],
            in_specs=[any_space] * 12,
            out_specs=[vmem] * 5,
            scratch_shapes=[
                pltpu.VMEM((OWN, CHIPS, ROWS, COLS), half),
                pltpu.VMEM((THEIRS, CHIPS, ROWS, COLS), half),
                pltpu.VMEM((CHIPS - 1, RING, ROWS, COLS), half),
                pltpu.VMEM((CHIPS - 1, RING, ROWS, COLS), half),
                pltpu.VMEM((SLOTS, ROWS, COLS), half),
                pltpu.VMEM((SLOTS, ROWS, COLS), full),
                pltpu.VMEM((SLOTS, ROWS, COLS), full),
                dma((OWN,)),
                dma,
                dma((THEIRS,)),
                pltpu.SemaphoreType.REGULAR,
                dma((CHIPS - 1, RING)),
                dma((CHIPS - 1, RING)),
                pltpu.SemaphoreType.REGULAR,
                dma((CHIPS - 1, RING)),
                dma((CHIPS - 1, RING)),
                pltpu.SemaphoreType.REGULAR,
                dma((3, SLOTS)),
                dma((3,)),
                dma((CHIPS - 1,)),
                dma((CHIPS - 1,)),
                dma,
                dma((CHIPS - 1, steps)),
                dma((CHIPS - 1, steps)),
                dma((3,)),
            ],
            compiler_params=pltpu.CompilerParams(collective_id=0, has_side_effects=True, vmem_limit_bytes=GRANT),
            name="sum_step_gather",
        )(*g, *w, *m, *v)
        held = [pltpu.with_memory_space_constraint(a, pltpu.VMEM) for a in got]
        return pl.pallas_call(
            functools.partial(finish, steps),
            out_shape=[pltpu.HBM(a.shape, a.dtype) for a in (*weights, *m, *v)],
            in_specs=[vmem] * 5,
            out_specs=[hbm] * 9,
            scratch_shapes=[dma((3,)), dma, dma],
            compiler_params=pltpu.CompilerParams(vmem_limit_bytes=GRANT),
            name="finish",
        )(*held)

    all_of, cut = P(None, None, None), P(None, "dp", None)
    return jax.shard_map(
        step,
        mesh=mesh,
        in_specs=(P(("rep", "dp"), None, None, None),) * 3 + (all_of,) * 3 + (cut,) * 6,
        out_specs=(P("rep", None, None),) * 3 + (P("rep", "dp", None),) * 6,
        check_vma=False,
    )
```

```python
import functools

import jax
import jax.numpy as jnp
from jax import lax
from jax.experimental import pallas as pl
from jax.experimental.pallas import tpu as pltpu
from jax.sharding import PartitionSpec as P

MESH = pl.DeviceIdType.MESH
CHIPS = 4
COLS = 1024
ROWS = 32
LAG = 1
AHEAD = 2
OWN = AHEAD + 3 * LAG + 1
SLOTS = 4
THEIRS = OWN + 2
GATHER = 8
RING = 6
GRANT = 9_400_000
BAND = 16


def piece(j, per, r, cols):
    layer = j // (per // 2)
    k = j % (per // 2)
    across = cols // COLS
    return layer, pl.multiple_of((k // across) * ROWS, ROWS), pl.multiple_of((k % across) * COLS, COLS)


def kernel(steps, *refs):
    g, w, m, v, wo = (refs[i : i + 3] for i in range(0, 15, 3))
    (m_new, v_new, own, theirs, right, left, w_in, m_in, v_in,
     own_sem, theirs_send, theirs_recv, theirs_free, right_send, right_recv, right_free, left_send, left_recv, left_free,
     in_sem, new_sem, relay_right, relay_left, relay_core, gather_right, gather_left, gather_core) = refs[15:]
    per = steps // 3
    rep, me = lax.axis_index("rep"), lax.axis_index("dp")
    z, c = me // 2, me % 2
    last = CHIPS - 1
    partner, up, down = (rep, me + 1 - 2 * c), (rep, me + 2), (rep, me - 2)

    barrier = pltpu.get_barrier_semaphore()
    pl.semaphore_signal(barrier, inc=1, device_id=partner, device_id_type=MESH)

    @pl.when(z < last)
    def _():
        pl.semaphore_signal(barrier, inc=1, device_id=up, device_id_type=MESH)

    @pl.when(z > 0)
    def _():
        pl.semaphore_signal(barrier, inc=1, device_id=down, device_id_type=MESH)

    pl.semaphore_wait(barrier, 1 + jnp.minimum(z, 1) + jnp.minimum(last - z, 1))

    def remote(src, dst, send, recv, to):
        return pltpu.make_async_remote_copy(src_ref=src, dst_ref=dst, send_sem=send, recv_sem=recv, device_id=to, device_id_type=MESH)

    def each_weight(j, do):
        for k in range(3):

            @pl.when((j >= k * per) & (j < (k + 1) * per))
            def _(k=k):
                layer, row, col = piece(j - k * per, per, m[k].shape[1], m[k].shape[2])
                do(k, layer, pl.ds(row, ROWS), pl.ds(col, COLS))

    def load_terms(j):
        t = j % THEIRS

        @pl.when(j >= THEIRS)
        def _():
            pl.semaphore_wait(theirs_free, 1)

        def do(k, layer, rows, cols):
            remote(g[k].at[layer, :, 1 - c, rows, cols], theirs.at[t], theirs_send, theirs_recv.at[t], partner).start()
            pltpu.make_async_copy(g[k].at[layer, :, c, rows, cols], own.at[j % OWN], own_sem.at[j % OWN]).start()

        each_weight(j, do)

    def load_state(j):
        s = j % SLOTS

        def do(k, layer, rows, cols):
            pltpu.make_async_copy(w[k].at[layer, z, c, rows, cols], w_in.at[s], in_sem.at[0, s]).start()
            pltpu.make_async_copy(m[k].at[layer, rows, cols], m_in.at[s], in_sem.at[1, s]).start()
            pltpu.make_async_copy(v[k].at[layer, rows, cols], v_in.at[s], in_sem.at[2, s]).start()

        each_weight(j, do)

    def bands(do):
        @pl.loop(0, ROWS // BAND)
        def _(t):
            do(pl.ds(pl.multiple_of(t * BAND, BAND), BAND))

    def forward(buf, slot, b, j, send, recv, to, first):
        q = j % RING

        @pl.when(first)
        def _():
            def do(r):
                total = own[j % OWN, b, r].astype(jnp.float32) + theirs[j % THEIRS, b, r].astype(jnp.float32)
                buf[slot, q, r] = total.astype(jnp.bfloat16)

            bands(do)

        @pl.when(jnp.logical_not(first))
        def _():
            remote(buf.at[slot, q], buf.at[slot, q], send.at[slot, q], recv.at[slot, q], to).wait_recv()

            def do(r):
                total = own[j % OWN, b, r].astype(jnp.float32) + theirs[j % THEIRS, b, r].astype(jnp.float32)
                buf[slot, q, r] = (total + buf[slot, q, r].astype(jnp.float32)).astype(jnp.bfloat16)

            bands(do)

        remote(buf.at[slot, q], buf.at[slot, q], send.at[slot, q], recv.at[slot, q], to).start()

    def step(j, k, layer, rows, cols, with_right, with_left):
        s, q = j % SLOTS, j % RING

        def do(r):
            total = own[j % OWN, z, r].astype(jnp.float32) + theirs[j % THEIRS, z, r].astype(jnp.float32)
            if with_right:
                total += right[jnp.maximum(z, 1) - 1, q, r].astype(jnp.float32)
            if with_left:
                total += left[jnp.minimum(z, 2), q, r].astype(jnp.float32)
            grad = total.astype(jnp.bfloat16).astype(jnp.float32)
            mean = 0.9 * m_in[s, r] + 0.1 * grad
            var = 0.95 * v_in[s, r] + 0.05 * grad * grad
            weight = w_in[s, r].astype(jnp.float32)
            change = mean * lax.rsqrt(var + 1e-8) + 0.1 * weight
            place = pl.ds(pl.multiple_of(rows.start + r.start, BAND), BAND)
            wo[k][layer, z, c, place, cols] = (weight - 0.02 * change).astype(jnp.bfloat16)
            m_new[j, r] = mean
            v_new[j, r] = var

        bands(do)

    def final(j):
        s, q = j % SLOTS, j % RING
        pltpu.make_async_copy(w[0].at[0, 0, 0, pl.ds(0, ROWS), pl.ds(0, COLS)], w_in.at[s], in_sem.at[0, s]).wait()
        pltpu.make_async_copy(m[0].at[0, pl.ds(0, ROWS), pl.ds(0, COLS)], m_in.at[s], in_sem.at[1, s]).wait()
        pltpu.make_async_copy(v[0].at[0, pl.ds(0, ROWS), pl.ds(0, COLS)], v_in.at[s], in_sem.at[2, s]).wait()

        @pl.when(z > 0)
        def _():
            slot = jnp.maximum(z, 1) - 1
            remote(right.at[slot, q], right.at[slot, q], right_send.at[slot, q], right_recv.at[slot, q], down).wait_recv()

        @pl.when(z < last)
        def _():
            slot = jnp.minimum(z, 2)
            remote(left.at[slot, q], left.at[slot, q], left_send.at[slot, q], left_recv.at[slot, q], up).wait_recv()

        def do(k, layer, rows, cols):
            @pl.when(z == 0)
            def _():
                step(j, k, layer, rows, cols, False, True)

            @pl.when(z == last)
            def _():
                step(j, k, layer, rows, cols, True, False)

            @pl.when((z > 0) & (z < last))
            def _():
                step(j, k, layer, rows, cols, True, True)

            here = wo[k].at[layer, z, c, rows, cols]

            @pl.when(z < last)
            def _():
                remote(here, here, new_sem.at[0], gather_right.at[jnp.minimum(z, 2), j % GATHER], up).start()

            @pl.when(z > 0)
            def _():
                remote(here, here, new_sem.at[1], gather_left.at[jnp.maximum(z, 1) - 1, j % GATHER], down).start()

            remote(here, here, new_sem.at[2], gather_core.at[k], partner).start()

        each_weight(j, do)

        @pl.when(j + 2 < steps)
        def _():
            load_state(j + 2)

    def retire(j):
        q = j % RING
        for n in range(last):
            b = last - n

            @pl.when(b > z)
            def _(b=b):
                remote(right.at[b - 1, q], right.at[b - 1, q], right_send.at[b - 1, q], right_recv.at[b - 1, q], up).wait_send()

            @pl.when(n < z)
            def _(n=n):
                remote(left.at[n, q], left.at[n, q], left_send.at[n, q], left_recv.at[n, q], down).wait_send()

        @pl.when((j < steps - RING) & (z > 0))
        def _():
            pl.semaphore_signal(right_free, inc=1, device_id=down, device_id_type=MESH)

        @pl.when((j < steps - RING) & (z < last))
        def _():
            pl.semaphore_signal(left_free, inc=1, device_id=up, device_id_type=MESH)

    def relay(b, j, slot, recv, sent, to, more):
        def do(k, layer, rows, cols):
            here = wo[k].at[layer, b, c, rows, cols]
            remote(here, here, sent.at[slot], recv.at[slot, j % GATHER], to).wait_recv()

            @pl.when(more)
            def _():
                remote(here, here, sent.at[slot], recv.at[slot, j % GATHER], to).start()

            remote(here, here, relay_core, gather_core.at[k], partner).start()

        each_weight(j, do)

    done_at = [LAG * max(b, last - b) for b in range(CHIPS)]
    mine = LAG * jnp.maximum(z, last - z)

    for j in range(AHEAD):
        load_terms(j)
    for j in range(2):
        load_state(j)

    def within(j):
        return (j >= 0) & (j < steps)

    @pl.loop(0, steps + 2 * last * LAG)
    def _(i):
        @pl.when(i + AHEAD < steps)
        def _():
            load_terms(i + AHEAD)

        @pl.when(i < steps)
        def _():
            pltpu.make_async_copy(own.at[i % OWN], own.at[i % OWN], own_sem.at[i % OWN]).wait()
            t = i % THEIRS
            remote(theirs.at[t], theirs.at[t], theirs_send, theirs_recv.at[t], partner).wait_recv()

        j_right = i - LAG * z
        j_left = i - LAG * (last - z)
        j_old = i - mine - 1

        @pl.when(within(j_old))
        def _():
            retire(j_old)

        @pl.when((j_right >= RING) & (j_right < steps) & (z < last))
        def _():
            pl.semaphore_wait(right_free, 1)

        @pl.when((j_left >= RING) & (j_left < steps) & (z > 0))
        def _():
            pl.semaphore_wait(left_free, 1)

        for n in range(last):
            b = last - n

            @pl.when(within(j_right) & (b > z))
            def _(b=b):
                forward(right, b - 1, b, j_right, right_send, right_recv, up, z == 0)

            @pl.when(within(j_left) & (n < z))
            def _(n=n):
                forward(left, n, n, j_left, left_send, left_recv, down, z == last)

        j_mine = i - mine

        @pl.when(within(j_mine))
        def _():
            final(j_mine)

        j_free = i - last * LAG

        @pl.when((j_free >= 0) & (j_free < steps - THEIRS))
        def _():
            pl.semaphore_signal(theirs_free, inc=1, device_id=partner, device_id_type=MESH)

        for n in range(last):
            b = last - n
            j = i - done_at[n] - LAG * (z - n)

            @pl.when(within(j) & (n < z))
            def _(n=n, j=j):
                relay(n, j, n, gather_right, relay_right, up, z < last)

            j = i - done_at[b] - LAG * (b - z)

            @pl.when(within(j) & (b > z))
            def _(b=b, j=j):
                relay(b, j, b - 1, gather_left, relay_left, down, z > 0)

    for k in range(3):
        sent = g[k].at[:, :, 1 - c]
        remote(sent, sent, theirs_send, gather_core.at[k], partner).wait_send()
        one = wo[k].at[:, 0, 0]
        for _ in range(last):
            remote(one, one, relay_core, gather_core.at[k], partner).wait_send()
        remote(one, one, new_sem.at[2], gather_core.at[k], partner).wait_send()

        @pl.when(z < last)
        def _():
            remote(one, one, new_sem.at[0], gather_core.at[k], up).wait_send()

        @pl.when(z > 0)
        def _():
            remote(one, one, new_sem.at[1], gather_core.at[k], down).wait_send()

        for n in range(last):
            b = last - n

            @pl.when((n < z) & (z < last))
            def _(n=n):
                remote(one, one, relay_right.at[n], gather_core.at[k], up).wait_send()

            @pl.when((b > z) & (z > 0))
            def _(b=b):
                remote(one, one, relay_left.at[b - 1], gather_core.at[k], down).wait_send()

    for k in range(3):
        arrived = wo[k].at[:, :, 1 - c]
        remote(arrived, arrived, theirs_send, gather_core.at[k], partner).wait_recv()


def finish(steps, *refs):
    w, m, v = refs[:3], refs[3], refs[4]
    wo, mo, vo = (refs[i : i + 3] for i in range(5, 14, 3))
    w_sem, m_sem, v_sem = refs[14:]
    per = steps // 3
    for k in range(3):
        layers, chips, cores, r, _ = w[k].shape

        @pl.loop(0, layers * chips * cores)
        def _(n, k=k, each=chips * cores, cores=cores, r=r):
            layer, b = n // each, n % each
            rows = pl.ds(pl.multiple_of(b * r, r), r)
            pltpu.make_async_copy(w[k].at[layer, b // cores, b % cores], wo[k].at[layer, rows], w_sem.at[k]).start()

        @pl.loop(0, per)
        def _(j, k=k):
            layer, row, col = piece(j, per, mo[k].shape[1], mo[k].shape[2])
            place = (layer, pl.ds(row, ROWS), pl.ds(col, COLS))
            pltpu.make_async_copy(m.at[k * per + j], mo[k].at[place], m_sem).start()
            pltpu.make_async_copy(v.at[k * per + j], vo[k].at[place], v_sem).start()

    for k in range(3):
        pltpu.make_async_copy(w[k], w[k], w_sem.at[k]).wait()
    pltpu.make_async_copy(m, m, m_sem).wait()
    pltpu.make_async_copy(v, v, v_sem).wait()


def solution(mesh):
    cores = mesh.shape["dp"] // CHIPS

    def step(*arrays):
        terms, weights, m, v = (arrays[i : i + 3] for i in (0, 3, 6, 9))
        steps = 3 * m[0].size // (ROWS * COLS)
        split = lambda a, one: a.reshape(one.shape[0], CHIPS, cores, *one.shape[1:])
        g = [split(a, one) for a, one in zip(terms, m, strict=True)]
        w = [split(a, one) for a, one in zip(weights, m, strict=True)]
        any_space, hbm, vmem = (pl.BlockSpec(memory_space=a) for a in (pl.ANY, pltpu.HBM, pltpu.VMEM))
        dma = pltpu.SemaphoreType.DMA
        half, full = jnp.bfloat16, jnp.float32
        state = (steps, ROWS, COLS)
        got = pl.pallas_call(
            functools.partial(kernel, steps),
            out_shape=[*(pltpu.VMEM(a.shape, a.dtype) for a in w), pltpu.VMEM(state, full), pltpu.VMEM(state, full)],
            in_specs=[any_space] * 12,
            out_specs=[vmem] * 5,
            scratch_shapes=[
                pltpu.VMEM((OWN, CHIPS, ROWS, COLS), half),
                pltpu.VMEM((THEIRS, CHIPS, ROWS, COLS), half),
                pltpu.VMEM((CHIPS - 1, RING, ROWS, COLS), half),
                pltpu.VMEM((CHIPS - 1, RING, ROWS, COLS), half),
                pltpu.VMEM((SLOTS, ROWS, COLS), half),
                pltpu.VMEM((SLOTS, ROWS, COLS), full),
                pltpu.VMEM((SLOTS, ROWS, COLS), full),
                dma((OWN,)),
                dma,
                dma((THEIRS,)),
                pltpu.SemaphoreType.REGULAR,
                dma((CHIPS - 1, RING)),
                dma((CHIPS - 1, RING)),
                pltpu.SemaphoreType.REGULAR,
                dma((CHIPS - 1, RING)),
                dma((CHIPS - 1, RING)),
                pltpu.SemaphoreType.REGULAR,
                dma((3, SLOTS)),
                dma((3,)),
                dma((CHIPS - 1,)),
                dma((CHIPS - 1,)),
                dma,
                dma((CHIPS - 1, GATHER)),
                dma((CHIPS - 1, GATHER)),
                dma((3,)),
            ],
            compiler_params=pltpu.CompilerParams(collective_id=0, has_side_effects=True, vmem_limit_bytes=GRANT),
            name="sum_step_gather",
        )(*g, *w, *m, *v)
        held = [pltpu.with_memory_space_constraint(a, pltpu.VMEM) for a in got]
        return pl.pallas_call(
            functools.partial(finish, steps),
            out_shape=[pltpu.HBM(a.shape, a.dtype) for a in (*weights, *m, *v)],
            in_specs=[vmem] * 5,
            out_specs=[hbm] * 9,
            scratch_shapes=[dma((3,)), dma, dma],
            compiler_params=pltpu.CompilerParams(vmem_limit_bytes=GRANT),
            name="finish",
        )(*held)

    all_of, cut = P(None, None, None), P(None, "dp", None)
    return jax.shard_map(
        step,
        mesh=mesh,
        in_specs=(P(("rep", "dp"), None, None, None),) * 3 + (all_of,) * 3 + (cut,) * 6,
        out_specs=(P("rep", None, None),) * 3 + (P("rep", "dp", None),) * 6,
        check_vma=False,
    )
```

```python
import functools

import jax
import jax.numpy as jnp
from jax import lax
from jax.experimental import pallas as pl
from jax.experimental.pallas import tpu as pltpu
from jax.sharding import PartitionSpec as P

MESH = pl.DeviceIdType.MESH
CHIPS = 4
COLS = 1024
ROWS = 32
LAG = 1
AHEAD = 2
OWN = AHEAD + 3 * LAG + 1
SLOTS = 3
THEIRS = OWN + 1
GATHER = 6
RING = 5
GRANT = 9_400_000
BAND = 16


def piece(j, per, r, cols):
    layer = j // (per // 2)
    k = j % (per // 2)
    across = cols // COLS
    return layer, pl.multiple_of((k // across) * ROWS, ROWS), pl.multiple_of((k % across) * COLS, COLS)


def kernel(steps, *refs):
    g, w, m, v, wo = (refs[i : i + 3] for i in range(0, 15, 3))
    (m_new, v_new, own, theirs, right, left, w_in, m_in, v_in,
     own_sem, theirs_send, theirs_recv, theirs_free, right_send, right_recv, right_free, left_send, left_recv, left_free,
     in_sem, new_sem, relay_right, relay_left, relay_core, gather_right, gather_left, gather_core) = refs[15:]
    per = steps // 3
    rep, me = lax.axis_index("rep"), lax.axis_index("dp")
    z, c = me // 2, me % 2
    last = CHIPS - 1
    partner, up, down = (rep, me + 1 - 2 * c), (rep, me + 2), (rep, me - 2)

    barrier = pltpu.get_barrier_semaphore()
    pl.semaphore_signal(barrier, inc=1, device_id=partner, device_id_type=MESH)

    @pl.when(z < last)
    def _():
        pl.semaphore_signal(barrier, inc=1, device_id=up, device_id_type=MESH)

    @pl.when(z > 0)
    def _():
        pl.semaphore_signal(barrier, inc=1, device_id=down, device_id_type=MESH)

    pl.semaphore_wait(barrier, 1 + jnp.minimum(z, 1) + jnp.minimum(last - z, 1))

    def remote(src, dst, send, recv, to):
        return pltpu.make_async_remote_copy(src_ref=src, dst_ref=dst, send_sem=send, recv_sem=recv, device_id=to, device_id_type=MESH)

    def each_weight(j, do):
        for k in range(3):

            @pl.when((j >= k * per) & (j < (k + 1) * per))
            def _(k=k):
                layer, row, col = piece(j - k * per, per, m[k].shape[1], m[k].shape[2])
                do(k, layer, pl.ds(row, ROWS), pl.ds(col, COLS))

    def load_terms(j):
        t = j % THEIRS

        @pl.when(j >= THEIRS)
        def _():
            pl.semaphore_wait(theirs_free, 1)

        def do(k, layer, rows, cols):
            remote(g[k].at[layer, :, 1 - c, rows, cols], theirs.at[t], theirs_send, theirs_recv.at[t], partner).start()
            pltpu.make_async_copy(g[k].at[layer, :, c, rows, cols], own.at[j % OWN], own_sem.at[j % OWN]).start()

        each_weight(j, do)

    def load_state(j):
        s = j % SLOTS

        def do(k, layer, rows, cols):
            pltpu.make_async_copy(w[k].at[layer, z, c, rows, cols], w_in.at[s], in_sem.at[0, s]).start()
            pltpu.make_async_copy(m[k].at[layer, rows, cols], m_in.at[s], in_sem.at[1, s]).start()
            pltpu.make_async_copy(v[k].at[layer, rows, cols], v_in.at[s], in_sem.at[2, s]).start()

        each_weight(j, do)

    def bands(do):
        @pl.loop(0, ROWS // BAND)
        def _(t):
            do(pl.ds(pl.multiple_of(t * BAND, BAND), BAND))

    def forward(buf, slot, b, j, send, recv, to, first):
        q = j % RING

        @pl.when(first)
        def _():
            def do(r):
                total = own[j % OWN, b, r].astype(jnp.float32) + theirs[j % THEIRS, b, r].astype(jnp.float32)
                buf[slot, q, r] = total.astype(jnp.bfloat16)

            bands(do)

        @pl.when(jnp.logical_not(first))
        def _():
            remote(buf.at[slot, q], buf.at[slot, q], send.at[slot, q], recv.at[slot, q], to).wait_recv()

            def do(r):
                total = own[j % OWN, b, r].astype(jnp.float32) + theirs[j % THEIRS, b, r].astype(jnp.float32)
                buf[slot, q, r] = (total + buf[slot, q, r].astype(jnp.float32)).astype(jnp.bfloat16)

            bands(do)

        remote(buf.at[slot, q], buf.at[slot, q], send.at[slot, q], recv.at[slot, q], to).start()

    def step(j, k, layer, rows, cols, with_right, with_left):
        s, q = j % SLOTS, j % RING

        def do(r):
            total = own[j % OWN, z, r].astype(jnp.float32) + theirs[j % THEIRS, z, r].astype(jnp.float32)
            if with_right:
                total += right[jnp.maximum(z, 1) - 1, q, r].astype(jnp.float32)
            if with_left:
                total += left[jnp.minimum(z, 2), q, r].astype(jnp.float32)
            grad = total.astype(jnp.bfloat16).astype(jnp.float32)
            mean = 0.9 * m_in[s, r] + 0.1 * grad
            var = 0.95 * v_in[s, r] + 0.05 * grad * grad
            weight = w_in[s, r].astype(jnp.float32)
            change = mean * lax.rsqrt(var + 1e-8) + 0.1 * weight
            place = pl.ds(pl.multiple_of(rows.start + r.start, BAND), BAND)
            wo[k][layer, z, c, place, cols] = (weight - 0.02 * change).astype(jnp.bfloat16)
            m_new[j, r] = mean
            v_new[j, r] = var

        bands(do)

    def final(j):
        s, q = j % SLOTS, j % RING
        pltpu.make_async_copy(w[0].at[0, 0, 0, pl.ds(0, ROWS), pl.ds(0, COLS)], w_in.at[s], in_sem.at[0, s]).wait()
        pltpu.make_async_copy(m[0].at[0, pl.ds(0, ROWS), pl.ds(0, COLS)], m_in.at[s], in_sem.at[1, s]).wait()
        pltpu.make_async_copy(v[0].at[0, pl.ds(0, ROWS), pl.ds(0, COLS)], v_in.at[s], in_sem.at[2, s]).wait()

        @pl.when(z > 0)
        def _():
            slot = jnp.maximum(z, 1) - 1
            remote(right.at[slot, q], right.at[slot, q], right_send.at[slot, q], right_recv.at[slot, q], down).wait_recv()

        @pl.when(z < last)
        def _():
            slot = jnp.minimum(z, 2)
            remote(left.at[slot, q], left.at[slot, q], left_send.at[slot, q], left_recv.at[slot, q], up).wait_recv()

        def do(k, layer, rows, cols):
            @pl.when(z == 0)
            def _():
                step(j, k, layer, rows, cols, False, True)

            @pl.when(z == last)
            def _():
                step(j, k, layer, rows, cols, True, False)

            @pl.when((z > 0) & (z < last))
            def _():
                step(j, k, layer, rows, cols, True, True)

            here = wo[k].at[layer, z, c, rows, cols]

            @pl.when(z < last)
            def _():
                remote(here, here, new_sem.at[0], gather_right.at[jnp.minimum(z, 2), j % GATHER], up).start()

            @pl.when(z > 0)
            def _():
                remote(here, here, new_sem.at[1], gather_left.at[jnp.maximum(z, 1) - 1, j % GATHER], down).start()

            remote(here, here, new_sem.at[2], gather_core.at[k], partner).start()

        each_weight(j, do)

        @pl.when(j + 2 < steps)
        def _():
            load_state(j + 2)

    def retire(j):
        q = j % RING
        for n in range(last):
            b = last - n

            @pl.when(b > z)
            def _(b=b):
                remote(right.at[b - 1, q], right.at[b - 1, q], right_send.at[b - 1, q], right_recv.at[b - 1, q], up).wait_send()

            @pl.when(n < z)
            def _(n=n):
                remote(left.at[n, q], left.at[n, q], left_send.at[n, q], left_recv.at[n, q], down).wait_send()

        @pl.when((j < steps - RING) & (z > 0))
        def _():
            pl.semaphore_signal(right_free, inc=1, device_id=down, device_id_type=MESH)

        @pl.when((j < steps - RING) & (z < last))
        def _():
            pl.semaphore_signal(left_free, inc=1, device_id=up, device_id_type=MESH)

    def relay(b, j, slot, recv, sent, to, more):
        def do(k, layer, rows, cols):
            here = wo[k].at[layer, b, c, rows, cols]
            remote(here, here, sent.at[slot], recv.at[slot, j % GATHER], to).wait_recv()

            @pl.when(more)
            def _():
                remote(here, here, sent.at[slot], recv.at[slot, j % GATHER], to).start()

            remote(here, here, relay_core, gather_core.at[k], partner).start()

        each_weight(j, do)

    done_at = [LAG * max(b, last - b) for b in range(CHIPS)]
    mine = LAG * jnp.maximum(z, last - z)

    for j in range(AHEAD):
        load_terms(j)
    for j in range(2):
        load_state(j)

    def within(j):
        return (j >= 0) & (j < steps)

    @pl.loop(0, steps + 2 * last * LAG)
    def _(i):
        @pl.when(i + AHEAD < steps)
        def _():
            load_terms(i + AHEAD)

        @pl.when(i < steps)
        def _():
            pltpu.make_async_copy(own.at[i % OWN], own.at[i % OWN], own_sem.at[i % OWN]).wait()
            t = i % THEIRS
            remote(theirs.at[t], theirs.at[t], theirs_send, theirs_recv.at[t], partner).wait_recv()

        j_right = i - LAG * z
        j_left = i - LAG * (last - z)
        j_old = i - mine - 1

        @pl.when(within(j_old))
        def _():
            retire(j_old)

        @pl.when((j_right >= RING) & (j_right < steps) & (z < last))
        def _():
            pl.semaphore_wait(right_free, 1)

        @pl.when((j_left >= RING) & (j_left < steps) & (z > 0))
        def _():
            pl.semaphore_wait(left_free, 1)

        for n in range(last):
            b = last - n

            @pl.when(within(j_right) & (b > z))
            def _(b=b):
                forward(right, b - 1, b, j_right, right_send, right_recv, up, z == 0)

            @pl.when(within(j_left) & (n < z))
            def _(n=n):
                forward(left, n, n, j_left, left_send, left_recv, down, z == last)

        j_mine = i - mine

        @pl.when(within(j_mine))
        def _():
            final(j_mine)

        j_free = i - last * LAG

        @pl.when((j_free >= 0) & (j_free < steps - THEIRS))
        def _():
            pl.semaphore_signal(theirs_free, inc=1, device_id=partner, device_id_type=MESH)

        for n in range(last):
            b = last - n
            j = i - done_at[n] - LAG * (z - n)

            @pl.when(within(j) & (n < z))
            def _(n=n, j=j):
                relay(n, j, n, gather_right, relay_right, up, z < last)

            j = i - done_at[b] - LAG * (b - z)

            @pl.when(within(j) & (b > z))
            def _(b=b, j=j):
                relay(b, j, b - 1, gather_left, relay_left, down, z > 0)

    for k in range(3):
        sent = g[k].at[:, :, 1 - c]
        remote(sent, sent, theirs_send, gather_core.at[k], partner).wait_send()
        one = wo[k].at[:, 0, 0]
        for _ in range(last):
            remote(one, one, relay_core, gather_core.at[k], partner).wait_send()
        remote(one, one, new_sem.at[2], gather_core.at[k], partner).wait_send()

        @pl.when(z < last)
        def _():
            remote(one, one, new_sem.at[0], gather_core.at[k], up).wait_send()

        @pl.when(z > 0)
        def _():
            remote(one, one, new_sem.at[1], gather_core.at[k], down).wait_send()

        for n in range(last):
            b = last - n

            @pl.when((n < z) & (z < last))
            def _(n=n):
                remote(one, one, relay_right.at[n], gather_core.at[k], up).wait_send()

            @pl.when((b > z) & (z > 0))
            def _(b=b):
                remote(one, one, relay_left.at[b - 1], gather_core.at[k], down).wait_send()

    for k in range(3):
        arrived = wo[k].at[:, :, 1 - c]
        remote(arrived, arrived, theirs_send, gather_core.at[k], partner).wait_recv()


def finish(steps, *refs):
    w, m, v = refs[:3], refs[3], refs[4]
    wo, mo, vo = (refs[i : i + 3] for i in range(5, 14, 3))
    w_sem, m_sem, v_sem = refs[14:]
    per = steps // 3
    for k in range(3):
        layers, chips, cores, r, _ = w[k].shape

        @pl.loop(0, layers * chips * cores)
        def _(n, k=k, each=chips * cores, cores=cores, r=r):
            layer, b = n // each, n % each
            rows = pl.ds(pl.multiple_of(b * r, r), r)
            pltpu.make_async_copy(w[k].at[layer, b // cores, b % cores], wo[k].at[layer, rows], w_sem.at[k]).start()

        @pl.loop(0, per)
        def _(j, k=k):
            layer, row, col = piece(j, per, mo[k].shape[1], mo[k].shape[2])
            place = (layer, pl.ds(row, ROWS), pl.ds(col, COLS))
            pltpu.make_async_copy(m.at[k * per + j], mo[k].at[place], m_sem).start()
            pltpu.make_async_copy(v.at[k * per + j], vo[k].at[place], v_sem).start()

    for k in range(3):
        pltpu.make_async_copy(w[k], w[k], w_sem.at[k]).wait()
    pltpu.make_async_copy(m, m, m_sem).wait()
    pltpu.make_async_copy(v, v, v_sem).wait()


def solution(mesh):
    cores = mesh.shape["dp"] // CHIPS

    def step(*arrays):
        terms, weights, m, v = (arrays[i : i + 3] for i in (0, 3, 6, 9))
        steps = 3 * m[0].size // (ROWS * COLS)
        split = lambda a, one: a.reshape(one.shape[0], CHIPS, cores, *one.shape[1:])
        g = [split(a, one) for a, one in zip(terms, m, strict=True)]
        w = [split(a, one) for a, one in zip(weights, m, strict=True)]
        any_space, hbm, vmem = (pl.BlockSpec(memory_space=a) for a in (pl.ANY, pltpu.HBM, pltpu.VMEM))
        dma = pltpu.SemaphoreType.DMA
        half, full = jnp.bfloat16, jnp.float32
        state = (steps, ROWS, COLS)
        got = pl.pallas_call(
            functools.partial(kernel, steps),
            out_shape=[*(pltpu.VMEM(a.shape, a.dtype) for a in w), pltpu.VMEM(state, full), pltpu.VMEM(state, full)],
            in_specs=[any_space] * 12,
            out_specs=[vmem] * 5,
            scratch_shapes=[
                pltpu.VMEM((OWN, CHIPS, ROWS, COLS), half),
                pltpu.VMEM((THEIRS, CHIPS, ROWS, COLS), half),
                pltpu.VMEM((CHIPS - 1, RING, ROWS, COLS), half),
                pltpu.VMEM((CHIPS - 1, RING, ROWS, COLS), half),
                pltpu.VMEM((SLOTS, ROWS, COLS), half),
                pltpu.VMEM((SLOTS, ROWS, COLS), full),
                pltpu.VMEM((SLOTS, ROWS, COLS), full),
                dma((OWN,)),
                dma,
                dma((THEIRS,)),
                pltpu.SemaphoreType.REGULAR,
                dma((CHIPS - 1, RING)),
                dma((CHIPS - 1, RING)),
                pltpu.SemaphoreType.REGULAR,
                dma((CHIPS - 1, RING)),
                dma((CHIPS - 1, RING)),
                pltpu.SemaphoreType.REGULAR,
                dma((3, SLOTS)),
                dma((3,)),
                dma((CHIPS - 1,)),
                dma((CHIPS - 1,)),
                dma,
                dma((CHIPS - 1, GATHER)),
                dma((CHIPS - 1, GATHER)),
                dma((3,)),
            ],
            compiler_params=pltpu.CompilerParams(collective_id=0, has_side_effects=True, vmem_limit_bytes=GRANT),
            name="sum_step_gather",
        )(*g, *w, *m, *v)
        held = [pltpu.with_memory_space_constraint(a, pltpu.VMEM) for a in got]
        return pl.pallas_call(
            functools.partial(finish, steps),
            out_shape=[pltpu.HBM(a.shape, a.dtype) for a in (*weights, *m, *v)],
            in_specs=[vmem] * 5,
            out_specs=[hbm] * 9,
            scratch_shapes=[dma((3,)), dma, dma],
            compiler_params=pltpu.CompilerParams(vmem_limit_bytes=GRANT),
            name="finish",
        )(*held)

    all_of, cut = P(None, None, None), P(None, "dp", None)
    return jax.shard_map(
        step,
        mesh=mesh,
        in_specs=(P(("rep", "dp"), None, None, None),) * 3 + (all_of,) * 3 + (cut,) * 6,
        out_specs=(P("rep", None, None),) * 3 + (P("rep", "dp", None),) * 6,
        check_vma=False,
    )
```
